32 devices in a mesh: energy: 16 (over z, y, core), cuts: 2 (over x).
Axes of the slice: x: 2, y: 2, z: 4, core: 2. Of those that a mesh axis runs over, the one named last changes fastest.
Arguments:
- green: bfloat16 [64, 2, 4, 128, 128], P('energy', 'cuts'), may hold values from -6 to 6
- offsets: int32 [4], replicated, may hold values from 1 to 2
- occupation: float32 [4], replicated, may hold values from 0.05 to 2
- coupling: bfloat16 [4, 3, 2, 128, 128], P(None, None, 'cuts'), may hold values from -0.25 to 0.25
Outputs:
- sigma: float32 [64, 2, 4, 128, 128], P('energy', 'cuts')
The draws below stay inside these ranges and needn't reach their ends.
All inputs are finite; a program needn't handle non-finite values.
Results may differ from the reference program's by a relative error of at most 0.0041.
Values may be sent and summed in bfloat16 or wider, within the bound.
A program may use at most 64 MiB of HBM per device.

```python
import math
import jax
import jax.numpy as jnp
from jax import lax

NO = 128
BR = 4
E_DEV = 4
OFFMAX = 2
NE = 64
NS = 2


def set_ends(values, own_key, low, top_value):
    shape = values.shape
    spot = [jax.random.randint(jax.random.fold_in(own_key, axis), (), 0, shape[axis]) for axis in range(len(shape))]
    values = values.at[tuple(spot)].set(low)
    longest = shape.index(max(shape))
    spot[longest] = (spot[longest] + 1) % shape[longest]
    return values.at[tuple(spot)].set(top_value)


def block_levels(stream_key, dims, cuts, least, largest):
    gain, own = 1.0, jax.random.fold_in(stream_key, 6)
    for dim, shards_of in cuts:
        steps = jnp.exp(jax.random.uniform(jax.random.fold_in(own, dim), (shards_of,), jnp.float32, least / len(cuts), largest / len(cuts)))
        gain = gain * jnp.repeat(steps, dims[dim] // shards_of).reshape([-1 if axis == dim else 1 for axis in range(len(dims))])
    return gain


def centred(own_key, shape, scale, most, pieces=(), kind=jnp.bfloat16):
    loudness = block_levels(own_key, shape, pieces, -0.22, 0.18) if pieces else 1.0
    entries = jax.random.normal(own_key, shape, jnp.float32) * scale * loudness
    return jnp.minimum(jnp.maximum(entries, -most), most).astype(kind)


def setup_inputs(seed: int = 0) -> dict:
    key_list = jax.random.split(jax.random.key(seed), 5)
    return {
        "green": centred(key_list[0], (NE, NS, 4, NO, NO), 1.0, 6.0, ((0, 16), (1, 2))),
        "offsets": set_ends(jax.random.randint(key_list[1], (BR,), 1, OFFMAX + 1), jax.random.fold_in(key_list[1], 1), 1, OFFMAX).astype(jnp.int32),
        "occupation": jnp.clip(jnp.exp(jax.random.uniform(key_list[2], (BR,), jnp.float32, math.log(0.05), math.log(2.0))), 0.05, 2.0),
        "coupling": centred(key_list[3], (BR, 3, NS, NO, NO), (4 * NO) ** -0.5, 0.25, ((2, 2),)),
    }


def self_energy(extended, offsets, occupation, coupling, energies, reach):
    slices = extended.shape[1] - 2
    orbitals = extended.shape[3]
    total = jnp.zeros((energies, slices, 4, orbitals, orbitals), jnp.float32)
    for branch in range(coupling.shape[0]):
        occupied = occupation[branch]
        lower = jnp.stack([occupied, occupied, occupied + 1.0, occupied + 1.0]).reshape(1, 1, 4, 1, 1)
        upper = jnp.stack([occupied + 1.0, occupied + 1.0, occupied, occupied]).reshape(1, 1, 4, 1, 1)
        below = lax.dynamic_slice_in_dim(extended, (reach - offsets[branch]).astype(jnp.int32), energies, 0)
        above = lax.dynamic_slice_in_dim(extended, (reach + offsets[branch]).astype(jnp.int32), energies, 0)
        mixed = (lower * below.astype(jnp.float32) + upper * above.astype(jnp.float32)).astype(jnp.bfloat16)
        for side in range(3):
            part = mixed[:, side:side + slices].astype(jnp.float32)
            block = coupling[branch, side].astype(jnp.float32)
            left = jnp.einsum("sab,escbd->escad", block, part, precision=lax.Precision.HIGHEST).astype(jnp.bfloat16)
            total = total + jnp.einsum("escad,sfd->escaf", left.astype(jnp.float32), block, precision=lax.Precision.HIGHEST)
    return total


def reference(green, offsets, occupation, coupling):
    padded = jnp.pad(green, ((OFFMAX, OFFMAX), (1, 1), (0, 0), (0, 0), (0, 0)))
    starts = jnp.arange(NE // E_DEV, dtype=jnp.int32) * E_DEV

    def one_block(start):
        window = lax.dynamic_slice_in_dim(padded, start.astype(jnp.int32), E_DEV + 2 * OFFMAX, 0)
        return self_energy(window, offsets, occupation, coupling, E_DEV, OFFMAX)

    blocks = lax.map(one_block, starts)
    return blocks.reshape(NE, NS, 4, NO, NO)
```

```python
import functools
import jax
import jax.numpy as jnp
from jax import lax
from jax.experimental import pallas as pl
from jax.experimental.pallas import tpu as pltpu
from jax.sharding import PartitionSpec as P

OFFMAX = 2
MESH = pl.DeviceIdType.MESH


def kernel(n_energy, n_cuts, slots, offsets, occupation, green, coupling, out,
           ext, kbuf, kt, acc, local_sem, k_sem, out_sem,
           own_send, own_recv, x_send, x_recv, relay_send, relay_recv):
    rank = lax.axis_index("energy")
    cut = lax.axis_index("cuts")
    count, parts = ext.shape[2] - 2 * OFFMAX, ext.shape[1]
    branches, width = kbuf.shape[0], kbuf.shape[2]
    reach = OFFMAX
    first = rank % 2
    second = 1 - first

    def at(energy, slice_):
        return {"energy": energy, "cuts": slice_}

    has = (rank > 0, rank < n_energy - 1)
    beside = (jnp.maximum(rank - 1, 0), jnp.minimum(rank + 1, n_energy - 1))
    if slots == 1:
        partners = [(1, 1, 1 - cut, None, 2 - 2 * cut)]
    elif slots == 2:
        partners = [
            (1, 2, jnp.maximum(cut - 1, 0), cut > 0, 0),
            (2, 1, jnp.minimum(cut + 1, n_cuts - 1), cut < n_cuts - 1, 2),
        ]
    else:
        partners = []

    def when(cond, do):
        if cond is None:
            do()
        else:
            pl.when(cond)(do)

    def exists(p):
        return jnp.where(p == 0, rank, n_energy - 1 - rank) > 0

    def toward(p):
        return jnp.clip(rank + 2 * p - 1, 0, n_energy - 1)

    def source(p):
        return (count - reach) * p + reach

    def landing(p):
        return (count + reach) * (1 - p)

    def own_copy(p, c):
        return pltpu.make_async_remote_copy(
            src_ref=ext.at[0, c, pl.ds(source(p), reach)],
            dst_ref=ext.at[0, c, pl.ds(landing(p), reach)],
            send_sem=own_send.at[p, c], recv_sem=own_recv.at[p, c],
            device_id=at(toward(p), cut), device_id_type=MESH)

    def relay_copy(slot, p, c):
        return pltpu.make_async_remote_copy(
            src_ref=ext.at[slot, c, pl.ds(source(p), reach)],
            dst_ref=ext.at[slot, c, pl.ds(landing(p), reach)],
            send_sem=relay_send.at[slot - 1, p, c], recv_sem=relay_recv.at[slot - 1, p, c],
            device_id=at(toward(p), cut), device_id_type=MESH)

    def x_copy(there, partner, p, c):
        return pltpu.make_async_remote_copy(
            src_ref=ext.at[0, c, pl.ds(source(p), reach)],
            dst_ref=ext.at[there, c, pl.ds(source(p), reach)],
            send_sem=x_send.at[there - 1, p, c], recv_sem=x_recv.at[there - 1, p, c],
            device_id=at(rank, partner), device_id_type=MESH)

    barrier = pltpu.get_barrier_semaphore()
    for p in range(2):
        pl.when(has[p])(functools.partial(
            pl.semaphore_signal, barrier, inc=1, device_id=at(beside[p], cut), device_id_type=MESH))
    for here, there, partner, cond, side in partners:
        when(cond, functools.partial(
            pl.semaphore_signal, barrier, inc=1, device_id=at(rank, partner), device_id_type=MESH))

    local = [pltpu.make_async_copy(green.at[:, 0, c], ext.at[0, c, pl.ds(reach, count)], local_sem.at[c])
             for c in range(parts)]
    for c in range(parts):
        local[c].start()
    k_copy = pltpu.make_async_copy(coupling.at[:, :, 0], kbuf, k_sem)
    k_copy.start()

    peers = sum(flag.astype(jnp.int32) for flag in has)
    for here, there, partner, cond, side in partners:
        peers = peers + (1 if cond is None else cond.astype(jnp.int32))
    pl.semaphore_wait(barrier, peers)

    order = [(0, 0)]
    for c in range(1, parts):
        order += [(0, c), (1, c - 1)]
    order += [(1, parts - 1)]
    waited = set()
    for which, c in order:
        if c not in waited:
            local[c].wait()
            waited.add(c)
        p = (first, second)[which]
        for here, there, partner, cond, side in partners:
            when(cond, lambda: x_copy(there, partner, p, c).start())
        if which == 0 and c < 2:
            for q in (first, second):
                pl.when(exists(q))(lambda: own_copy(q, c).start())

    @pl.when(rank == 0)
    def _():
        ext[:, :, pl.ds(0, reach)] = jnp.zeros((slots + 1, parts, reach, width, width), ext.dtype)

    @pl.when(rank == n_energy - 1)
    def _():
        ext[:, :, pl.ds(count + reach, reach)] = jnp.zeros((slots + 1, parts, reach, width, width), ext.dtype)

    k_copy.wait()
    for s in range(kbuf.shape[1]):
        for b in range(branches):
            kt[s, b * width:(b + 1) * width, :] = kbuf[b, s].T

    def forward(which, c):
        p = (first, second)[which]
        for here, there, partner, cond, side in partners:
            def go():
                x_copy(here, partner, p, c).wait_recv()
                pl.when(exists(p))(lambda: relay_copy(here, p, c).start())
            when(cond, go)

    def send_own(c):
        for q in (first, second):
            pl.when(exists(q))(lambda: own_copy(q, c).start())

    def own_ready(c):
        for p in range(2):
            pl.when(has[p])(lambda: own_copy(1 - p, c).wait_recv())

    steps = parts * (slots + 1)
    plan = {}
    position = 0
    for k in range(parts):
        todo = []
        if position < len(order):
            todo.append(order[position])
            position += 1
        plan[k] = todo
    k = parts
    if partners:
        plan[k] = [order[position]] if position < len(order) else []
        position += 1
        while position < len(order):
            k = min(k + 1, 2 * parts - 1)
            take = 2 if len(order) - position > 1 else 1
            plan.setdefault(k, [])
            plan[k] += order[position:position + take]
            position += take

    def compute(slot, side, c):
        values = [ext[slot, c, e].astype(jnp.float32) for e in range(count + 2 * reach)]
        lefts = []
        for b in range(branches):
            n = occupation[b]
            w = offsets[b]
            lesser = c < parts // 2
            lower = jnp.where(lesser, n, n + 1.0)
            upper = jnp.where(lesser, n + 1.0, n)
            low = [jnp.where(w == d, lower, 0.0) for d in range(1, reach + 1)]
            up = [jnp.where(w == d, upper, 0.0) for d in range(1, reach + 1)]
            mixed = []
            for e in range(count):
                total = None
                for d in range(1, reach + 1):
                    term = low[d - 1] * values[reach + e - d] + up[d - 1] * values[reach + e + d]
                    total = term if total is None else total + term
                mixed.append(total.astype(jnp.bfloat16))
            lefts.append(jnp.dot(kbuf[b, side], jnp.concatenate(mixed, axis=1),
                                 preferred_element_type=jnp.float32).astype(jnp.bfloat16))
        rows = [jnp.concatenate([left[:, e * width:(e + 1) * width] for left in lefts], axis=1)
                for e in range(count)]
        return jnp.dot(jnp.concatenate(rows, axis=0), kt[side], preferred_element_type=jnp.float32)

    def out_copy(c):
        return pltpu.make_async_copy(acc.at[c], out.at[:, 0, c], out_sem.at[c])

    def step(t, carry):
        slot = t // parts
        c = t % parts
        for k, todo in plan.items():
            if todo or k + 2 < parts:
                @pl.when(t == k)
                def _():
                    for which, part in todo:
                        forward(which, part)
                    if k + 2 < parts:
                        send_own(k + 2)

        @pl.when(slot == 0)
        def _():
            own_ready(c)

        runs = slot == 0
        side = jnp.where(slot == 0, 1, 0)
        for here, there, partner, cond, which_side in partners:
            side = jnp.where(slot == here, which_side, side)
            mine = slot == here
            if cond is not None:
                mine = jnp.logical_and(mine, cond)
            runs = jnp.logical_or(runs, mine)

            @pl.when(mine)
            def _():
                for p in range(2):
                    pl.when(has[p])(lambda: relay_copy(here, 1 - p, c).wait_recv())

        def work():
            sums = compute(slot, side, c)

            @pl.when(slot == 0)
            def _():
                for e in range(count):
                    acc[c, e] = sums[e * width:(e + 1) * width]

            @pl.when(slot > 0)
            def _():
                for e in range(count):
                    acc[c, e] += sums[e * width:(e + 1) * width]

        if slots == 2:
            pl.when(runs)(work)
        else:
            work()

        @pl.when(slot == slots)
        def _():
            out_copy(c).start()
        return carry

    lax.fori_loop(0, steps, step, 0)

    for c in range(parts):
        for p in range(2):
            pl.when(has[p])(lambda: own_copy(p, c).wait_send())
            for here, there, partner, cond, side in partners:
                when(cond, lambda: x_copy(there, partner, p, c).wait_send())
                both = has[p] if cond is None else jnp.logical_and(cond, has[p])
                pl.when(both)(lambda: relay_copy(here, p, c).wait_send())
    for c in range(parts):
        out_copy(c).wait()


def body(n_energy, n_cuts, green, offsets, occupation, coupling):
    count, slices, parts, width, _ = green.shape
    branches, sides = coupling.shape[:2]
    assert slices == 1 and count == 2 * OFFMAX
    slots = min(n_cuts - 1, 2)
    sems = max(slots, 1)
    dma = pltpu.SemaphoreType.DMA
    return pl.pallas_call(
        functools.partial(kernel, n_energy, n_cuts, slots),
        out_shape=jax.ShapeDtypeStruct(green.shape, jnp.float32),
        in_specs=[
            pl.BlockSpec(memory_space=pltpu.SMEM),
            pl.BlockSpec(memory_space=pltpu.SMEM),
            pl.BlockSpec(memory_space=pl.ANY),
            pl.BlockSpec(memory_space=pl.ANY),
        ],
        out_specs=pl.BlockSpec(memory_space=pl.ANY),
        scratch_shapes=[
            pltpu.VMEM((slots + 1, parts, count + 2 * OFFMAX, width, width), jnp.bfloat16),
            pltpu.VMEM((branches, sides, width, width), jnp.bfloat16),
            pltpu.VMEM((sides, branches * width, width), jnp.bfloat16),
            pltpu.VMEM((parts, count, width, width), jnp.float32),
            dma((parts,)),
            dma,
            dma((parts,)),
            dma((2, parts)),
            dma((2, parts)),
            dma((sems, 2, parts)),
            dma((sems, 2, parts)),
            dma((sems, 2, parts)),
            dma((sems, 2, parts)),
        ],
        compiler_params=pltpu.CompilerParams(collective_id=0, has_side_effects=True),
    )(offsets, occupation, green, coupling)


def solution(mesh):
    sizes = dict(mesh.shape)
    in_specs = (P("energy", "cuts", None, None, None), P(), P(), P(None, None, "cuts", None, None))
    out_specs = P("energy", "cuts", None, None, None)
    return jax.shard_map(
        functools.partial(body, sizes["energy"], sizes["cuts"]),
        mesh=mesh, in_specs=in_specs, out_specs=out_specs, check_vma=False)
```

```python
import functools
import jax
import jax.numpy as jnp
from jax import lax
from jax.experimental import pallas as pl
from jax.experimental.pallas import tpu as pltpu
from jax.sharding import PartitionSpec as P

OFFMAX = 2
MESH = pl.DeviceIdType.MESH


def kernel(n_energy, n_cuts, slots, offsets, occupation, green, coupling, acc,
           ext, kbuf, kt, local_sem, k_sem,
           own_send, own_recv, x_send, x_recv, relay_send, relay_recv):
    rank = lax.axis_index("energy")
    cut = lax.axis_index("cuts")
    count, parts = ext.shape[2] - 2 * OFFMAX, ext.shape[1]
    branches, width = kbuf.shape[0], kbuf.shape[2]
    reach = OFFMAX
    first = rank % 2
    second = 1 - first

    def at(energy, slice_):
        return {"energy": energy, "cuts": slice_}

    has = (rank > 0, rank < n_energy - 1)
    beside = (jnp.maximum(rank - 1, 0), jnp.minimum(rank + 1, n_energy - 1))
    if slots == 1:
        partners = [(1, 1, 1 - cut, None, 2 - 2 * cut)]
    elif slots == 2:
        partners = [
            (1, 2, jnp.maximum(cut - 1, 0), cut > 0, 0),
            (2, 1, jnp.minimum(cut + 1, n_cuts - 1), cut < n_cuts - 1, 2),
        ]
    else:
        partners = []

    def when(cond, do):
        if cond is None:
            do()
        else:
            pl.when(cond)(do)

    def exists(p):
        return jnp.where(p == 0, rank, n_energy - 1 - rank) > 0

    def toward(p):
        return jnp.clip(rank + 2 * p - 1, 0, n_energy - 1)

    def source(p):
        return (count - reach) * p + reach

    def landing(p):
        return (count + reach) * (1 - p)

    def own_copy(p, c):
        return pltpu.make_async_remote_copy(
            src_ref=ext.at[0, c, pl.ds(source(p), reach)],
            dst_ref=ext.at[0, c, pl.ds(landing(p), reach)],
            send_sem=own_send.at[p, c], recv_sem=own_recv.at[p, c],
            device_id=at(toward(p), cut), device_id_type=MESH)

    def relay_copy(slot, p, c):
        return pltpu.make_async_remote_copy(
            src_ref=ext.at[slot, c, pl.ds(source(p), reach)],
            dst_ref=ext.at[slot, c, pl.ds(landing(p), reach)],
            send_sem=relay_send.at[slot - 1, p, c], recv_sem=relay_recv.at[slot - 1, p, c],
            device_id=at(toward(p), cut), device_id_type=MESH)

    def x_copy(there, partner, p, c):
        return pltpu.make_async_remote_copy(
            src_ref=ext.at[0, c, pl.ds(source(p), reach)],
            dst_ref=ext.at[there, c, pl.ds(source(p), reach)],
            send_sem=x_send.at[there - 1, p, c], recv_sem=x_recv.at[there - 1, p, c],
            device_id=at(rank, partner), device_id_type=MESH)

    barrier = pltpu.get_barrier_semaphore()
    for p in range(2):
        pl.when(has[p])(functools.partial(
            pl.semaphore_signal, barrier, inc=1, device_id=at(beside[p], cut), device_id_type=MESH))
    for here, there, partner, cond, side in partners:
        when(cond, functools.partial(
            pl.semaphore_signal, barrier, inc=1, device_id=at(rank, partner), device_id_type=MESH))

    local = [pltpu.make_async_copy(green.at[:, 0, c], ext.at[0, c, pl.ds(reach, count)], local_sem.at[c])
             for c in range(parts)]
    for c in range(parts):
        local[c].start()
    k_copy = pltpu.make_async_copy(coupling.at[:, :, 0], kbuf, k_sem)
    k_copy.start()

    peers = sum(flag.astype(jnp.int32) for flag in has)
    for here, there, partner, cond, side in partners:
        peers = peers + (1 if cond is None else cond.astype(jnp.int32))
    pl.semaphore_wait(barrier, peers)

    order = [(0, 0)]
    for c in range(1, parts):
        order += [(0, c), (1, c - 1)]
    order += [(1, parts - 1)]
    waited = set()
    for which, c in order:
        if c not in waited:
            local[c].wait()
            waited.add(c)
        p = (first, second)[which]
        for here, there, partner, cond, side in partners:
            when(cond, lambda: x_copy(there, partner, p, c).start())
        if which == 0 and c < 2:
            for q in (first, second):
                pl.when(exists(q))(lambda: own_copy(q, c).start())

    @pl.when(rank == 0)
    def _():
        ext[:, :, pl.ds(0, reach)] = jnp.zeros((slots + 1, parts, reach, width, width), ext.dtype)

    @pl.when(rank == n_energy - 1)
    def _():
        ext[:, :, pl.ds(count + reach, reach)] = jnp.zeros((slots + 1, parts, reach, width, width), ext.dtype)

    k_copy.wait()
    for s in range(kbuf.shape[1]):
        for b in range(branches):
            kt[s, b * width:(b + 1) * width, :] = kbuf[b, s].T

    def forward(which, c):
        p = (first, second)[which]
        for here, there, partner, cond, side in partners:
            def go():
                x_copy(here, partner, p, c).wait_recv()
                pl.when(exists(p))(lambda: relay_copy(here, p, c).start())
            when(cond, go)

    def send_own(c):
        for q in (first, second):
            pl.when(exists(q))(lambda: own_copy(q, c).start())

    def own_ready(c):
        for p in range(2):
            pl.when(has[p])(lambda: own_copy(1 - p, c).wait_recv())

    steps = parts * (slots + 1)
    plan = {}
    position = 0
    for k in range(parts):
        todo = []
        if position < len(order):
            todo.append(order[position])
            position += 1
        plan[k] = todo
    k = parts
    if partners:
        plan[k] = [order[position]] if position < len(order) else []
        position += 1
        while position < len(order):
            k = min(k + 1, 2 * parts - 1)
            take = 2 if len(order) - position > 1 else 1
            plan.setdefault(k, [])
            plan[k] += order[position:position + take]
            position += take

    def compute(slot, side, c):
        values = [ext[slot, c, e].astype(jnp.float32) for e in range(count + 2 * reach)]
        lefts = []
        for b in range(branches):
            n = occupation[b]
            w = offsets[b]
            lesser = c < parts // 2
            lower = jnp.where(lesser, n, n + 1.0)
            upper = jnp.where(lesser, n + 1.0, n)
            low = [jnp.where(w == d, lower, 0.0) for d in range(1, reach + 1)]
            up = [jnp.where(w == d, upper, 0.0) for d in range(1, reach + 1)]
            mixed = []
            for e in range(count):
                total = None
                for d in range(1, reach + 1):
                    term = low[d - 1] * values[reach + e - d] + up[d - 1] * values[reach + e + d]
                    total = term if total is None else total + term
                mixed.append(total.astype(jnp.bfloat16))
            lefts.append(jnp.dot(kbuf[b, side], jnp.concatenate(mixed, axis=1),
                                 preferred_element_type=jnp.float32).astype(jnp.bfloat16))
        rows = [jnp.concatenate([left[:, e * width:(e + 1) * width] for left in lefts], axis=1)
                for e in range(count)]
        return jnp.dot(jnp.concatenate(rows, axis=0), kt[side], preferred_element_type=jnp.float32)

    def step(t, carry):
        slot = t // parts
        c = t % parts
        for k, todo in plan.items():
            if todo or k + 2 < parts:
                @pl.when(t == k)
                def _():
                    for which, part in todo:
                        forward(which, part)
                    if k + 2 < parts:
                        send_own(k + 2)

        @pl.when(slot == 0)
        def _():
            own_ready(c)

        runs = slot == 0
        side = jnp.where(slot == 0, 1, 0)
        for here, there, partner, cond, which_side in partners:
            side = jnp.where(slot == here, which_side, side)
            mine = slot == here
            if cond is not None:
                mine = jnp.logical_and(mine, cond)
            runs = jnp.logical_or(runs, mine)

            @pl.when(mine)
            def _():
                for p in range(2):
                    pl.when(has[p])(lambda: relay_copy(here, 1 - p, c).wait_recv())

        def work():
            sums = compute(slot, side, c)

            @pl.when(slot == 0)
            def _():
                for e in range(count):
                    acc[c, e] = sums[e * width:(e + 1) * width]

            @pl.when(slot > 0)
            def _():
                for e in range(count):
                    acc[c, e] += sums[e * width:(e + 1) * width]

        if slots == 2:
            pl.when(runs)(work)
        else:
            work()

        return carry

    lax.fori_loop(0, steps, step, 0)

    for c in range(parts):
        for p in range(2):
            pl.when(has[p])(lambda: own_copy(p, c).wait_send())
            for here, there, partner, cond, side in partners:
                when(cond, lambda: x_copy(there, partner, p, c).wait_send())
                both = has[p] if cond is None else jnp.logical_and(cond, has[p])
                pl.when(both)(lambda: relay_copy(here, p, c).wait_send())


def write_out(sums, out, sem):
    copies = [pltpu.make_async_copy(sums.at[c], out.at[:, 0, c], sem.at[c]) for c in range(sums.shape[0])]
    for copy in copies:
        copy.start()
    for copy in copies:
        copy.wait()


def body(n_energy, n_cuts, green, offsets, occupation, coupling):
    count, slices, parts, width, _ = green.shape
    branches, sides = coupling.shape[:2]
    assert slices == 1 and count == 2 * OFFMAX
    slots = min(n_cuts - 1, 2)
    sems = max(slots, 1)
    dma = pltpu.SemaphoreType.DMA
    sums = pl.pallas_call(
        functools.partial(kernel, n_energy, n_cuts, slots),
        out_shape=pltpu.VMEM((parts, count, width, width), jnp.float32),
        in_specs=[
            pl.BlockSpec(memory_space=pltpu.SMEM),
            pl.BlockSpec(memory_space=pltpu.SMEM),
            pl.BlockSpec(memory_space=pl.ANY),
            pl.BlockSpec(memory_space=pl.ANY),
        ],
        out_specs=pl.BlockSpec(memory_space=pltpu.VMEM),
        scratch_shapes=[
            pltpu.VMEM((slots + 1, parts, count + 2 * OFFMAX, width, width), jnp.bfloat16),
            pltpu.VMEM((branches, sides, width, width), jnp.bfloat16),
            pltpu.VMEM((sides, branches * width, width), jnp.bfloat16),
            dma((parts,)),
            dma,
            dma((2, parts)),
            dma((2, parts)),
            dma((sems, 2, parts)),
            dma((sems, 2, parts)),
            dma((sems, 2, parts)),
            dma((sems, 2, parts)),
        ],
        compiler_params=pltpu.CompilerParams(collective_id=0, has_side_effects=True),
    )(offsets, occupation, green, coupling)
    return pl.pallas_call(
        write_out,
        out_shape=jax.ShapeDtypeStruct(green.shape, jnp.float32),
        in_specs=[pl.BlockSpec(memory_space=pltpu.VMEM)],
        out_specs=pl.BlockSpec(memory_space=pl.ANY),
        scratch_shapes=[dma((parts,))],
    )(pltpu.with_memory_space_constraint(sums, pltpu.VMEM))


def solution(mesh):
    sizes = dict(mesh.shape)
    in_specs = (P("energy", "cuts", None, None, None), P(), P(), P(None, None, "cuts", None, None))
    out_specs = P("energy", "cuts", None, None, None)
    return jax.shard_map(
        functools.partial(body, sizes["energy"], sizes["cuts"]),
        mesh=mesh, in_specs=in_specs, out_specs=out_specs, check_vma=False)
```

```python
import functools
import jax
import jax.numpy as jnp
from jax import lax
from jax.experimental import pallas as pl
from jax.experimental.pallas import tpu as pltpu
from jax.sharding import PartitionSpec as P

OFFMAX = 2
MESH = pl.DeviceIdType.MESH


def kernel(n_energy, n_cuts, slots, offsets_in, occupation_in, green, coupling, acc,
           offsets, occupation, ext, kbuf, kt, small_sem, local_sem, k_sem,
           own_send, own_recv, x_send, x_recv, relay_send, relay_recv):
    rank = lax.axis_index("energy")
    cut = lax.axis_index("cuts")
    count, parts = ext.shape[2] - 2 * OFFMAX, ext.shape[1]
    branches, width = kbuf.shape[0], kbuf.shape[2]
    reach = OFFMAX
    first = rank % 2
    second = 1 - first

    def at(energy, slice_):
        return {"energy": energy, "cuts": slice_}

    has = (rank > 0, rank < n_energy - 1)
    beside = (jnp.maximum(rank - 1, 0), jnp.minimum(rank + 1, n_energy - 1))
    if slots == 1:
        partners = [(1, 1, 1 - cut, None, 2 - 2 * cut)]
    elif slots == 2:
        partners = [
            (1, 2, jnp.maximum(cut - 1, 0), cut > 0, 0),
            (2, 1, jnp.minimum(cut + 1, n_cuts - 1), cut < n_cuts - 1, 2),
        ]
    else:
        partners = []

    def when(cond, do):
        if cond is None:
            do()
        else:
            pl.when(cond)(do)

    def exists(p):
        return jnp.where(p == 0, rank, n_energy - 1 - rank) > 0

    def toward(p):
        return jnp.clip(rank + 2 * p - 1, 0, n_energy - 1)

    def source(p):
        return (count - reach) * p + reach

    def landing(p):
        return (count + reach) * (1 - p)

    def own_copy(p, c):
        return pltpu.make_async_remote_copy(
            src_ref=ext.at[0, c, pl.ds(source(p), reach)],
            dst_ref=ext.at[0, c, pl.ds(landing(p), reach)],
            send_sem=own_send.at[p, c], recv_sem=own_recv.at[p, c],
            device_id=at(toward(p), cut), device_id_type=MESH)

    def relay_copy(slot, p, c):
        return pltpu.make_async_remote_copy(
            src_ref=ext.at[slot, c, pl.ds(source(p), reach)],
            dst_ref=ext.at[slot, c, pl.ds(landing(p), reach)],
            send_sem=relay_send.at[slot - 1, p, c], recv_sem=relay_recv.at[slot - 1, p, c],
            device_id=at(toward(p), cut), device_id_type=MESH)

    def x_copy(there, partner, p, c):
        return pltpu.make_async_remote_copy(
            src_ref=ext.at[0, c, pl.ds(source(p), reach)],
            dst_ref=ext.at[there, c, pl.ds(source(p), reach)],
            send_sem=x_send.at[there - 1, p, c], recv_sem=x_recv.at[there - 1, p, c],
            device_id=at(rank, partner), device_id_type=MESH)

    barrier = pltpu.get_barrier_semaphore()
    for p in range(2):
        pl.when(has[p])(functools.partial(
            pl.semaphore_signal, barrier, inc=1, device_id=at(beside[p], cut), device_id_type=MESH))
    for here, there, partner, cond, side in partners:
        when(cond, functools.partial(
            pl.semaphore_signal, barrier, inc=1, device_id=at(rank, partner), device_id_type=MESH))

    local = [pltpu.make_async_copy(green.at[:, 0, c], ext.at[0, c, pl.ds(reach, count)], local_sem.at[c])
             for c in range(parts)]
    for c in range(parts):
        local[c].start()
    k_copy = pltpu.make_async_copy(coupling.at[:, :, 0], kbuf, k_sem)
    k_copy.start()
    small = [pltpu.make_async_copy(offsets_in, offsets, small_sem.at[0]),
             pltpu.make_async_copy(occupation_in, occupation, small_sem.at[1])]
    for copy in small:
        copy.start()

    peers = sum(flag.astype(jnp.int32) for flag in has)
    for here, there, partner, cond, side in partners:
        peers = peers + (1 if cond is None else cond.astype(jnp.int32))
    pl.semaphore_wait(barrier, peers)

    order = [(0, 0)]
    for c in range(1, parts):
        order += [(0, c), (1, c - 1)]
    order += [(1, parts - 1)]
    waited = set()
    for which, c in order:
        if c not in waited:
            local[c].wait()
            waited.add(c)
        p = (first, second)[which]
        for here, there, partner, cond, side in partners:
            when(cond, lambda: x_copy(there, partner, p, c).start())
        if which == 0:
            for q in (first, second):
                pl.when(exists(q))(lambda: own_copy(q, c).start())

    @pl.when(rank == 0)
    def _():
        ext[:, :, pl.ds(0, reach)] = jnp.zeros((slots + 1, parts, reach, width, width), ext.dtype)

    @pl.when(rank == n_energy - 1)
    def _():
        ext[:, :, pl.ds(count + reach, reach)] = jnp.zeros((slots + 1, parts, reach, width, width), ext.dtype)

    k_copy.wait()
    for copy in small:
        copy.wait()
    for s in range(kbuf.shape[1]):
        for b in range(branches):
            kt[s, b * width:(b + 1) * width, :] = kbuf[b, s].T

    def forward(which, c):
        p = (first, second)[which]
        for here, there, partner, cond, side in partners:
            def go():
                x_copy(here, partner, p, c).wait_recv()
                pl.when(exists(p))(lambda: relay_copy(here, p, c).start())
            when(cond, go)

    def own_ready(c):
        for p in range(2):
            pl.when(has[p])(lambda: own_copy(1 - p, c).wait_recv())

    steps = parts * (slots + 1)
    last = 2 * parts - 2
    plan = {}
    for position, item in enumerate(order if partners else []):
        plan.setdefault(min(position, last), []).append(item)

    def compute(slot, side, c):
        values = [ext[slot, c, e].astype(jnp.float32) for e in range(count + 2 * reach)]
        lefts = []
        for b in range(branches):
            n = occupation[b]
            w = offsets[b]
            lesser = c < parts // 2
            lower = jnp.where(lesser, n, n + 1.0)
            upper = jnp.where(lesser, n + 1.0, n)
            low = [jnp.where(w == d, lower, 0.0) for d in range(1, reach + 1)]
            up = [jnp.where(w == d, upper, 0.0) for d in range(1, reach + 1)]
            mixed = []
            for e in range(count):
                total = None
                for d in range(1, reach + 1):
                    term = low[d - 1] * values[reach + e - d] + up[d - 1] * values[reach + e + d]
                    total = term if total is None else total + term
                mixed.append(total.astype(jnp.bfloat16))
            lefts.append(jnp.dot(kbuf[b, side], jnp.concatenate(mixed, axis=1),
                                 preferred_element_type=jnp.float32).astype(jnp.bfloat16))
        rows = [jnp.concatenate([left[:, e * width:(e + 1) * width] for left in lefts], axis=1)
                for e in range(count)]
        return jnp.dot(jnp.concatenate(rows, axis=0), kt[side], preferred_element_type=jnp.float32)

    def step(t, carry):
        slot = t // parts
        c = t % parts
        for k, todo in plan.items():
            @pl.when(t == k)
            def _():
                for which, part in todo:
                    forward(which, part)

        @pl.when(slot == 0)
        def _():
            own_ready(c)

        runs = slot == 0
        side = jnp.where(slot == 0, 1, 0)
        for here, there, partner, cond, which_side in partners:
            side = jnp.where(slot == here, which_side, side)
            mine = slot == here
            if cond is not None:
                mine = jnp.logical_and(mine, cond)
            runs = jnp.logical_or(runs, mine)

            @pl.when(mine)
            def _():
                for p in range(2):
                    pl.when(has[p])(lambda: relay_copy(here, 1 - p, c).wait_recv())

        def work():
            sums = compute(slot, side, c)

            @pl.when(slot == 0)
            def _():
                for e in range(count):
                    acc[c, e] = sums[e * width:(e + 1) * width]

            @pl.when(slot > 0)
            def _():
                for e in range(count):
                    acc[c, e] += sums[e * width:(e + 1) * width]

        if slots == 2:
            pl.when(runs)(work)
        else:
            work()

        return carry

    lax.fori_loop(0, steps, step, 0)

    for c in range(parts):
        for p in range(2):
            pl.when(has[p])(lambda: own_copy(p, c).wait_send())
            for here, there, partner, cond, side in partners:
                when(cond, lambda: x_copy(there, partner, p, c).wait_send())
                both = has[p] if cond is None else jnp.logical_and(cond, has[p])
                pl.when(both)(lambda: relay_copy(here, p, c).wait_send())


def write_out(sums, out, sem):
    copies = [pltpu.make_async_copy(sums.at[c], out.at[:, 0, c], sem.at[c]) for c in range(sums.shape[0])]
    for copy in copies:
        copy.start()
    for copy in copies:
        copy.wait()


def body(n_energy, n_cuts, green, offsets, occupation, coupling):
    count, slices, parts, width, _ = green.shape
    branches, sides = coupling.shape[:2]
    assert slices == 1 and count == 2 * OFFMAX
    slots = min(n_cuts - 1, 2)
    sems = max(slots, 1)
    dma = pltpu.SemaphoreType.DMA
    sums = pl.pallas_call(
        functools.partial(kernel, n_energy, n_cuts, slots),
        out_shape=pltpu.VMEM((parts, count, width, width), jnp.float32),
        in_specs=[
            pl.BlockSpec(memory_space=pl.ANY),
            pl.BlockSpec(memory_space=pl.ANY),
            pl.BlockSpec(memory_space=pl.ANY),
            pl.BlockSpec(memory_space=pl.ANY),
        ],
        out_specs=pl.BlockSpec(memory_space=pltpu.VMEM),
        scratch_shapes=[
            pltpu.SMEM(offsets.shape, offsets.dtype),
            pltpu.SMEM(occupation.shape, occupation.dtype),
            pltpu.VMEM((slots + 1, parts, count + 2 * OFFMAX, width, width), jnp.bfloat16),
            pltpu.VMEM((branches, sides, width, width), jnp.bfloat16),
            pltpu.VMEM((sides, branches * width, width), jnp.bfloat16),
            dma((2,)),
            dma((parts,)),
            dma,
            dma((2, parts)),
            dma((2, parts)),
            dma((sems, 2, parts)),
            dma((sems, 2, parts)),
            dma((sems, 2, parts)),
            dma((sems, 2, parts)),
        ],
        compiler_params=pltpu.CompilerParams(collective_id=0, has_side_effects=True),
    )(offsets, occupation, green, coupling)
    return pl.pallas_call(
        write_out,
        out_shape=jax.ShapeDtypeStruct(green.shape, jnp.float32),
        in_specs=[pl.BlockSpec(memory_space=pltpu.VMEM)],
        out_specs=pl.BlockSpec(memory_space=pl.ANY),
        scratch_shapes=[dma((parts,))],
    )(pltpu.with_memory_space_constraint(sums, pltpu.VMEM))


def solution(mesh):
    sizes = dict(mesh.shape)
    in_specs = (P("energy", "cuts", None, None, None), P(), P(), P(None, None, "cuts", None, None))
    out_specs = P("energy", "cuts", None, None, None)
    return jax.shard_map(
        functools.partial(body, sizes["energy"], sizes["cuts"]),
        mesh=mesh, in_specs=in_specs, out_specs=out_specs, check_vma=False)
```
